32 devices in a mesh: groups: 2 (over y), ep: 16 (over z, x, core).
Axes of the slice: x: 2, y: 2, z: 4, core: 2. Of those that a mesh axis runs over, the one named last changes fastest.
Arguments:
- residual_in: bfloat16 [64, 4096], P(('groups', 'ep')), parts along dimension 0, may hold values from -6 to 6
- queries: bfloat16 [64, 4096], P(('groups', 'ep')), parts along dimension 0, may hold values from -144 to 144
- fresh_keys: bfloat16 [64, 512], P(('groups', 'ep')), parts along dimension 0, may hold values from -6 to 6
- fresh_values: bfloat16 [64, 512], P(('groups', 'ep')), parts along dimension 0, may hold values from -6 to 6
- stored_keys: bfloat16 [64, 256, 512], P(('groups', 'ep')), parts along dimension 0, may hold values from -6 to 6
- stored_values: bfloat16 [64, 256, 512], P(('groups', 'ep')), parts along dimension 0, may hold values from -6 to 6
- context_len: int32 [64], P(('groups', 'ep')), parts along dimension 0, may hold values from 2 to 256
- norm_gain: float32 [4096], replicated, may hold values from 0.5 to 1.5
- expert_ids: int32 [64, 2], P(('groups', 'ep')), parts along dimension 0, may hold values from 0 to 3, all different within a row; in each aligned block of 2 rows (0 to 1, 2 to 3, ...) at most 2 rows name the same one
- expert_gates: bfloat16 [64, 2], P(('groups', 'ep')), parts along dimension 0, may hold values from 0.19921875 to 1
- gate_weight: bfloat16 [4096, 49152], P(None, 'ep'), may hold values from -0.09375 to 0.09375
- up_weight: bfloat16 [4096, 49152], P(None, 'ep'), may hold values from -0.09375 to 0.09375
- down_weight: bfloat16 [49152, 4096], P('ep'), may hold values from -0.0546875 to 0.0546875
Outputs:
- mixed: bfloat16 [64, 4096], P(('groups', 'ep')), parts along dimension 0
The draws below stay inside these ranges and needn't reach their ends.
There are 2 independent parts, one for each index of `groups`. The reference program is written for one: setup_inputs(seed, part) draws one part's arguments, and reference() takes and returns one part's arrays. A program takes and returns all parts, laid end to end along the dimension named above; an argument that names none is the same for every part. Nothing has to cross between parts.
Inputs may be any that keep to these rules, and one draw needn't show every extreme that they name: `expert_ids`: each row names 2 different experts. In the rows of one device no expert is named more than 2 times, and in some device's rows some expert is named exactly 2 times.
All inputs are finite; a program needn't handle non-finite values.
Results may differ from the reference program's by a relative error of at most 0.006.
Values may be sent and summed in bfloat16 or wider, within the bound.
A program may use at most 128 MiB of HBM per device.

```python
import math
import jax
import jax.numpy as jnp
import numpy as np
from jax import lax

QUERY_HEADS = 32
KEY_VALUE_HEADS = 4
HEAD_WIDTH = 128
D = 4096
KVD = 512
EXPERTS = 4
FF = 12288
TOP = 2
REQ = 2
CACHED_POSITIONS = 256
CAP = 2
REQUEST_COUNT = 32
N_EP = 16


def shared_draw(key):
    random_seed_key = jax.random.fold_in(key, 7)
    key_tensor = jnp.clip(jax.random.normal(jax.random.fold_in(random_seed_key, 1), (REQUEST_COUNT, CACHED_POSITIONS, KEY_VALUE_HEADS * HEAD_WIDTH), jnp.float32), -6.0, 6.0)
    query_array = jnp.clip(jax.random.normal(jax.random.fold_in(random_seed_key, 2), (REQUEST_COUNT, QUERY_HEADS * HEAD_WIDTH), jnp.float32), -6.0, 6.0)
    return (key_tensor, query_array)


def draw_queries(key, part):
    return shared_draw(key)[1].astype(jnp.bfloat16)


def draw_stored_keys(key, part):
    return shared_draw(key)[0].astype(jnp.bfloat16)


def set_ends(array, key, least, high):
    dims = array.shape
    index_at = [jax.random.randint(jax.random.fold_in(key, axis), (), 0, dims[axis]) for axis in range(len(dims))]
    array = array.at[tuple(index_at)].set(least)
    longest = dims.index(max(dims))
    index_at[longest] = (index_at[longest] + 1) % dims[longest]
    return array.at[tuple(index_at)].set(high)


def steps_of(key, shape, cuts, low, high):
    def one(axis_at, blocks):
        heights = jax.random.uniform(jax.random.fold_in(jax.random.fold_in(key, 6), axis_at), (blocks,), jnp.float32, low / len(cuts), high / len(cuts))
        return jnp.repeat(jnp.exp(heights), shape[axis_at] // blocks).reshape((-1,) + (1,) * (len(shape) - axis_at - 1))

    loudness = one(*cuts[0])
    for cut in cuts[1:]:
        loudness = loudness * one(*cut)
    return loudness


def assign_block(stream_key, own, number, rows, number_of, top, limit, slope):
    sequence = jax.random.permutation(stream_key, number_of)
    packed, usual = load_shares(number_of, rows * top, limit, slope, True), load_shares(number_of, rows * top, limit, slope, False)
    places = jnp.arange(number_of)

    def named(lengths, rotation):
        used = int((lengths > 0).sum())
        fixed = max(1, used // 4)
        passed = fixed + (places - fixed + rotation * (used - fixed)) % max(1, number_of - fixed)
        return jnp.zeros((number_of,), jnp.int32).at[sequence[jnp.where(places < fixed, places, passed)]].set(jnp.asarray(lengths, jnp.int32))

    lengths = jnp.where(number % 4 == 0, named(packed, number // 4), named(usual, number - number // 4 - 1))
    mixed = jax.random.permutation(jax.random.fold_in(own, 3), number_of)
    source_of, receiver = mixed[0:number_of // 2 * 2:2], mixed[1:number_of // 2 * 2:2]
    slack = jnp.minimum(lengths[source_of] - 1, limit - lengths[receiver]) // 2
    slack = jnp.where((source_of == sequence[0]) | (receiver == sequence[0]) | (lengths[receiver] == 0), 0, jnp.maximum(slack, 0))
    passed = jax.random.randint(jax.random.fold_in(own, 4), (number_of // 2,), 0, 1 << 20) % (slack + 1)
    lengths = lengths.at[source_of].add(-passed).at[receiver].add(passed)
    items = jnp.searchsorted(jnp.cumsum(lengths), jnp.arange(rows * top), side="right").astype(jnp.int32)
    grid = items.reshape(top, rows).T
    grid = grid[jax.random.permutation(jax.random.fold_in(own, 1), rows)]
    rotation = jax.random.randint(jax.random.fold_in(own, 2), (rows, 1), 0, top)
    return jnp.take_along_axis(grid, (jnp.arange(top)[None, :] + rotation) % top, axis=1)


def load_shares(amount, total, most, slope, full):
    loads = [(1 << 20) // math.isqrt(rank ** slope) + 1 for rank in range(1, amount + 1)]
    largest = most if full else min(most, max(-(-total // amount), total * loads[0] // sum(loads)))
    least = 1 if total - largest >= amount - 1 else 0
    counts, spare = [largest] + [least] * (amount - 1), total - largest - least * (amount - 1)
    while spare > 0:
        movable = [i for i in range(1, amount) if counts[i] < largest] or [i for i in range(1, amount) if counts[i] < most]
        whole, remaining = sum([loads[i] for i in movable]), spare
        for i in movable:
            more = min(most - counts[i], max(1, remaining * loads[i] // whole), spare)
            counts[i] = counts[i] + more
            spare = spare - more
    return np.array(counts)


def noise(rng, extent, deviation, limit, pieces=(), held_as=jnp.bfloat16):
    factor_of = steps_of(rng, extent, pieces, -0.22, 0.18) if pieces else 1.0
    values = jax.random.normal(rng, extent, jnp.float32) * deviation * factor_of
    return jnp.minimum(jnp.maximum(values, -limit), limit).astype(held_as)


def setup_inputs(seed: int = 0, part: int = 0) -> dict:
    streams_of = jax.random.split(jax.random.key(seed), 14)
    part_keys = jax.random.split(jax.random.fold_in(streams_of[13], part), 14)
    residual_in = noise(part_keys[0], (REQUEST_COUNT, D), 1.0, 6.0, ((0, 16),))
    queries = draw_queries(jax.random.fold_in(jax.random.fold_in(streams_of[13], part), 71), part)
    fresh_keys = noise(part_keys[2], (REQUEST_COUNT, KVD), 1.0, 6.0, ((0, 16),))
    fresh_values = noise(part_keys[3], (REQUEST_COUNT, KVD), 1.0, 6.0, ((0, 16),))
    stored_keys = draw_stored_keys(jax.random.fold_in(jax.random.fold_in(streams_of[13], part), 71), part)
    stored_values = noise(part_keys[5], (REQUEST_COUNT, CACHED_POSITIONS, KVD), 1.0, 6.0, ((0, 16),))
    context_len = set_ends(jax.random.randint(part_keys[6], (REQUEST_COUNT,), 2, CACHED_POSITIONS + 1), jax.random.fold_in(part_keys[6], 1), 2, CACHED_POSITIONS).astype(jnp.int32)
    norm_gain = jnp.clip(1.0 + 0.1 * jax.random.normal(streams_of[7], (D,), jnp.float32), 0.5, 1.5)
    expert_ids_keys = jax.random.split(jax.random.fold_in(part_keys[8], 1), REQUEST_COUNT // REQ)
    expert_ids_turns = jax.random.permutation(jax.random.fold_in(part_keys[8], 3), REQUEST_COUNT // REQ)
    expert_ids = jax.vmap(lambda own, number: assign_block(jax.random.fold_in(part_keys[8], 2), own, number, REQ, EXPERTS, TOP, CAP, 2))(expert_ids_keys, expert_ids_turns).reshape((REQUEST_COUNT, TOP))
    expert_gates = jnp.clip(0.19921875 + 0.80078125 * jax.random.uniform(part_keys[9], (REQUEST_COUNT, TOP), jnp.float32) ** steps_of(part_keys[9], (REQUEST_COUNT, TOP), ((0, 16),), -0.2, 0.2), 0.19921875, 1.0).astype(jnp.bfloat16)
    gate_weight = noise(streams_of[10], (D, EXPERTS * FF), D ** -0.5, 0.09375, ((1, 16),))
    up_weight = noise(streams_of[11], (D, EXPERTS * FF), D ** -0.5, 0.09375, ((1, 16),))
    down_weight = noise(streams_of[12], (EXPERTS * FF, D), FF ** -0.5, 0.0546875, ((0, 16),))
    return dict(residual_in=residual_in, queries=queries, fresh_keys=fresh_keys, fresh_values=fresh_values, stored_keys=stored_keys, stored_values=stored_values, context_len=context_len, norm_gain=norm_gain, expert_ids=expert_ids, expert_gates=expert_gates, gate_weight=gate_weight, up_weight=up_weight, down_weight=down_weight)


def attend(queries, fresh_keys, fresh_values, stored_keys, stored_values, context_len):
    request_batch = queries.shape[0]
    position_index = stored_keys.shape[1]
    query_group_width = QUERY_HEADS // KEY_VALUE_HEADS
    logit_scale = 1.0 / math.sqrt(HEAD_WIDTH)
    query_head_rows = queries.astype(jnp.float32).reshape(request_batch, KEY_VALUE_HEADS, query_group_width, HEAD_WIDTH)
    key_head_rows = stored_keys.astype(jnp.float32).reshape(request_batch, position_index, KEY_VALUE_HEADS, HEAD_WIDTH)
    value_head_rows = stored_values.astype(jnp.float32).reshape(request_batch, position_index, KEY_VALUE_HEADS, HEAD_WIDTH)
    scores = jnp.einsum('rkgd,rlkd->rkgl', query_head_rows, key_head_rows) * logit_scale
    self_score = jnp.einsum('mteh,mth->mte', query_head_rows, fresh_keys.astype(jnp.float32).reshape(request_batch, KEY_VALUE_HEADS, HEAD_WIDTH)) * logit_scale
    valid_mask = (lax.broadcasted_iota(jnp.int32, (request_batch, position_index), 1) < context_len.astype(jnp.int32)[:, None])[:, None, None, :]
    row_max = jnp.maximum(lax.optimization_barrier(jnp.max(jnp.where(valid_mask, scores, -1e+30), axis=3)), self_score)
    exp_scores = jnp.where(valid_mask, jnp.exp(scores - row_max[..., None]), 0.0)
    own_exp = jnp.exp(self_score - row_max)
    denominator = lax.optimization_barrier(jnp.sum(exp_scores, axis=3)) + own_exp
    weights = (exp_scores / denominator[..., None]).astype(jnp.bfloat16)
    self_weight = (own_exp / denominator).astype(jnp.bfloat16)
    value_mixture = jnp.einsum('rkgl,rlkd->rkgd', weights.astype(jnp.float32), value_head_rows)
    value_mixture = value_mixture + self_weight.astype(jnp.float32)[..., None] * fresh_values.astype(jnp.float32).reshape(request_batch, KEY_VALUE_HEADS, 1, HEAD_WIDTH)
    return value_mixture.reshape(request_batch, QUERY_HEADS * HEAD_WIDTH)

def slot_places(id_block, gate_block):
    flat_ids = id_block.reshape(-1).astype(jnp.int32)
    onehot = (flat_ids[:, None] == jnp.arange(EXPERTS, dtype=jnp.int32)[None, :]).astype(jnp.int32)
    earlier = jnp.cumsum(onehot, axis=0) - onehot
    slot_index = lax.optimization_barrier(jnp.sum(earlier * onehot, axis=1))
    where_to = (flat_ids * CAP + slot_index).reshape(id_block.shape)
    matches = where_to[:, :, None] == jnp.arange(EXPERTS * CAP, dtype=jnp.int32)[None, None, :]
    return lax.optimization_barrier(jnp.sum(jnp.where(matches, gate_block.astype(jnp.float32)[:, :, None], jnp.float32(0.0)), axis=1))

def reference(residual_in, queries, fresh_keys, fresh_values, stored_keys, stored_values, context_len, norm_gain, expert_ids, expert_gates, gate_weight, up_weight, down_weight):
    attended = attend(queries, fresh_keys, fresh_values, stored_keys, stored_values, context_len)
    residual = residual_in.astype(jnp.float32) + attended
    normed = (residual * lax.rsqrt(lax.optimization_barrier(jnp.mean(residual * residual, axis=1, keepdims=True)) + 1e-05) * norm_gain).astype(jnp.bfloat16)
    blocks = N_EP
    placement = jax.vmap(slot_places)(expert_ids.reshape(blocks, REQ, TOP), expert_gates.reshape(blocks, REQ, TOP))
    chosen = (placement != 0.0).astype(jnp.float32)
    token_blocks = normed.astype(jnp.float32).reshape(blocks, REQ, D)

    def one_expert(expert):
        start = (expert * CAP).astype(jnp.int32)
        my_columns = lax.dynamic_slice_in_dim(chosen, start, CAP, 2)
        gate_scale = lax.optimization_barrier(jnp.sum(lax.dynamic_slice_in_dim(placement, start, CAP, 2), axis=1))
        dispatched = jnp.einsum('brc,brd->bcd', my_columns, token_blocks).astype(jnp.bfloat16).reshape(blocks * CAP, D)
        first_unit = (expert * FF).astype(jnp.int32)
        gate_proj = jnp.dot(dispatched, lax.dynamic_slice_in_dim(gate_weight, first_unit, FF, 1), preferred_element_type=jnp.float32)
        up_proj = jnp.dot(dispatched, lax.dynamic_slice_in_dim(up_weight, first_unit, FF, 1), preferred_element_type=jnp.float32)
        hidden = (jax.nn.silu(gate_proj) * up_proj).astype(jnp.bfloat16)
        down_proj = jnp.dot(hidden, lax.dynamic_slice_in_dim(down_weight, first_unit, FF, 0), preferred_element_type=jnp.float32)
        return down_proj.reshape(blocks, CAP, D) * gate_scale[:, :, None]
    expert_outputs = lax.map(one_expert, jnp.arange(EXPERTS, dtype=jnp.int32))
    per_slot = jnp.transpose(expert_outputs, (1, 0, 2, 3)).reshape(blocks, EXPERTS * CAP, D)
    expert_mix = jnp.einsum('brj,bjd->brd', chosen, per_slot, precision=lax.Precision.HIGHEST).reshape(blocks * REQ, D)
    return (residual + expert_mix).astype(jnp.bfloat16)
```

```python
import functools
import math

import jax
import jax.numpy as jnp
from jax import lax
from jax.experimental import pallas as pl
from jax.experimental.pallas import tpu as pltpu
from jax.sharding import PartitionSpec as P

KEY_VALUE_HEADS = 4
HEAD_WIDTH = 128
EXPERTS = 4
CHUNK = 512
RING = 5
EARLY = 3
IN_CHUNK = 512
OUT_CHUNK = 512
LAG = 2

norm_eps = 1e-05
MESH = pl.DeviceIdType.MESH


def attend(q_ref, fk_ref, fv_ref, k_ref, v_ref, ctx_ref, q_rows, att):
    reqs, features = q_ref.shape
    positions = k_ref.shape[1]
    heads = features // HEAD_WIDTH
    group = heads // KEY_VALUE_HEADS
    scale = 1.0 / math.sqrt(HEAD_WIDTH)
    q = q_ref[...].astype(jnp.float32)
    fk = fk_ref[...].astype(jnp.float32)
    fv = fv_ref[...].astype(jnp.float32)
    for r in range(reqs):
        for h in range(heads):
            q_rows[r * heads + h : r * heads + h + 1, :] = q[
                r : r + 1, h * HEAD_WIDTH : (h + 1) * HEAD_WIDTH
            ]
    scores, own, valid = [], [], []
    position = lax.broadcasted_iota(jnp.int32, (heads, positions), 1)
    for r in range(reqs):
        valid.append(position < ctx_ref[r])
        for j in range(KEY_VALUE_HEADS):
            rows = slice(r * heads + j * group, r * heads + (j + 1) * group)
            cols = slice(j * HEAD_WIDTH, (j + 1) * HEAD_WIDTH)
            qj = q_rows[rows, :]
            scores.append(
                lax.dot_general(
                    qj.astype(jnp.bfloat16),
                    k_ref[r, :, cols],
                    (((1,), (1,)), ((), ())),
                    preferred_element_type=jnp.float32,
                )
            )
            own.append(jnp.sum(qj * fk[r : r + 1, cols], axis=1, keepdims=True))
    ok = jnp.concatenate(valid, axis=0)
    s = jnp.concatenate(scores, axis=0) * scale
    o = jnp.concatenate(own, axis=0) * scale
    m = jnp.maximum(jnp.max(jnp.where(ok, s, -1e30), axis=1, keepdims=True), o)
    e = jnp.where(ok, jnp.exp(s - m), 0.0)
    oe = jnp.exp(o - m)
    total = jnp.sum(e, axis=1, keepdims=True) + oe
    w = (e / total).astype(jnp.bfloat16)
    ow = (oe / total).astype(jnp.bfloat16).astype(jnp.float32)
    for r in range(reqs):
        for j in range(KEY_VALUE_HEADS):
            rows = slice(r * heads + j * group, r * heads + (j + 1) * group)
            cols = slice(j * HEAD_WIDTH, (j + 1) * HEAD_WIDTH)
            mixed = jnp.dot(w[rows], v_ref[r, :, cols], preferred_element_type=jnp.float32)
            mixed = mixed + ow[rows] * fv[r : r + 1, cols]
            for g in range(group):
                h = j * group + g
                att[r : r + 1, h * HEAD_WIDTH : (h + 1) * HEAD_WIDTH] = mixed[g : g + 1, :]


def shared_kernel(groups, n, *refs):
    small_hbm, refs = refs[:10], refs[10:]
    small, refs = refs[4:14], refs[:4] + refs[14:]
    (
        wg_hbm,
        wu_hbm,
        wd_hbm,
        out_ref,
        wg,
        wu,
        wd,
        q_rows,
        residual,
        xs,
        xd,
        xf,
        x32,
        acc_g,
        acc_u,
        hidden,
        keep,
        ps,
        pr,
        ys,
        yr,
        in_sem,
        g_sem,
        u_sem,
        d_sem,
        x_send,
        x_recv,
        f_send,
        f_recv,
        p_send,
        p_recv,
        y_send,
        y_recv,
    ) = refs
    ctx_ref, res_ref, q_ref, fk_ref, fv_ref, gain_ref, ids_ref, gates_ref, k_buf, v_buf = small
    g, e = lax.axis_index("groups"), lax.axis_index("ep")
    per_group = n // 2
    chips = groups * per_group
    core = lax.rem(e, 2)
    chip = g * per_group + e // 2
    partner = {"groups": g, "ep": e + 1 - 2 * core}
    reqs, features = res_ref.shape
    k_steps, chunk, units = wg.shape
    j_steps, _, out_chunk = wd.shape
    rows = chips * reqs

    def across(d):
        q = lax.rem(chip + d, chips)
        return {"groups": q // per_group, "ep": lax.rem(q, per_group) * 2 + 1 - core}

    loads = [
        pltpu.make_async_copy(source, target, in_sem.at[i])
        for i, (source, target) in enumerate(zip(small_hbm, small))
    ]
    for load in loads:
        load.start()

    first = pl.multiple_of(g * units, 128)

    def gate_copy(step):
        at = pl.ds(pl.multiple_of(step * chunk, chunk), chunk)
        return pltpu.make_async_copy(wg_hbm.at[at, pl.ds(first, units)], wg.at[step], g_sem.at[step])

    def up_copy(step):
        at = pl.ds(pl.multiple_of(step * chunk, chunk), chunk)
        return pltpu.make_async_copy(wu_hbm.at[at, pl.ds(first, units)], wu.at[step], u_sem.at[step])

    def down_copy(step):
        at = pl.ds(pl.multiple_of(step * out_chunk, out_chunk), out_chunk)
        return pltpu.make_async_copy(wd_hbm.at[pl.ds(first, units), at], wd.at[step], d_sem.at[step])

    @pl.loop(0, k_steps)
    def _(step):
        gate_copy(step).start(priority=1)
        up_copy(step).start(priority=1)

    @pl.loop(0, j_steps)
    def _(step):
        down_copy(step).start(priority=1)

    barrier = pltpu.get_barrier_semaphore()

    @pl.loop(0, chips)
    def _(d):
        pl.semaphore_signal(barrier, inc=1, device_id=across(d), device_id_type=MESH)

    acc_g[...] = jnp.zeros_like(acc_g)
    acc_u[...] = jnp.zeros_like(acc_u)
    for load in loads:
        load.wait()
    attend(q_ref, fk_ref, fv_ref, k_buf, v_buf, ctx_ref, q_rows, residual)
    full = res_ref[...].astype(jnp.float32) + residual[...]
    residual[...] = full
    factor = lax.rsqrt(jnp.mean(full * full, axis=1, keepdims=True) + norm_eps)
    normed = (full * factor * gain_ref[...]).astype(jnp.bfloat16)
    for k in range(k_steps):
        xs[k] = normed[:, k * chunk : (k + 1) * chunk]

    pl.semaphore_wait(barrier, chips)

    @pl.loop(0, k_steps)
    def _(k):
        @pl.loop(0, chips)
        def _(d):
            pltpu.make_async_remote_copy(
                src_ref=xs.at[k],
                dst_ref=xd.at[k, chip],
                send_sem=x_send.at[k],
                recv_sem=x_recv.at[k],
                device_id=across(d),
                device_id_type=MESH,
            ).start()

    def wait_for(ref, sem):
        pltpu.make_async_copy(ref, ref, sem).wait()

    def forward(k):
        return pltpu.make_async_remote_copy(
            src_ref=xd.at[k],
            dst_ref=xf.at[k],
            send_sem=f_send.at[k],
            recv_sem=f_recv.at[k],
            device_id=partner,
            device_id_type=MESH,
        )

    def pass_on(k):
        wait_for(xd.at[k], x_recv.at[k])
        forward(k).start()

    pass_on(0)

    @pl.loop(0, k_steps)
    def _(k):
        @pl.when(k + 1 < k_steps)
        def _():
            pass_on(k + 1)

        forward(k).wait_recv()
        for q in range(chips):
            x32[reqs * q : reqs * (q + 1), :] = xd[k, q].astype(jnp.float32)
            x32[rows + reqs * q : rows + reqs * (q + 1), :] = xf[k, q].astype(jnp.float32)
        x = x32[...].astype(jnp.bfloat16)
        gate_copy(k).wait()
        acc_g[...] += jnp.dot(x, wg[k], preferred_element_type=jnp.float32)
        up_copy(k).wait()
        acc_u[...] += jnp.dot(x, wu[k], preferred_element_type=jnp.float32)

    gate = acc_g[...]
    hidden[...] = (gate / (1.0 + jnp.exp(-gate)) * acc_u[...]).astype(jnp.bfloat16)

    def give(j):
        return pltpu.make_async_remote_copy(
            src_ref=ps.at[j],
            dst_ref=pr.at[j],
            send_sem=p_send.at[j],
            recv_sem=p_recv.at[j],
            device_id=partner,
            device_id_type=MESH,
        )

    def send_back(j):
        give(j).wait_recv()
        both = (keep[j] + pr[j].astype(jnp.float32)).astype(jnp.bfloat16)
        for q in range(chips):
            ys[j, q] = both[reqs * q : reqs * (q + 1)]

        @pl.loop(0, chips)
        def _(d):
            pltpu.make_async_remote_copy(
                src_ref=ys.at[j, lax.rem(chip + d, chips)],
                dst_ref=yr.at[j, chip],
                send_sem=y_send.at[j],
                recv_sem=y_recv.at[j],
                device_id=across(d),
                device_id_type=MESH,
            ).start()

    lag = min(LAG, j_steps)

    @pl.loop(0, j_steps)
    def _(j):
        down_copy(j).wait()
        part = jnp.dot(hidden[...], wd[j], preferred_element_type=jnp.float32)
        keep[j] = part[0:rows]
        ps[j] = part[rows:].astype(jnp.bfloat16)
        give(j).start()

        @pl.when(j >= lag)
        def _():
            send_back(j - lag)

    @pl.loop(j_steps - lag, j_steps)
    def _(j):
        send_back(j)

    ids = ids_ref[...]
    gates = gates_ref[...].astype(jnp.float32)
    per_expert = per_group // EXPERTS
    weights = []
    for expert in range(EXPERTS):
        weights.append(jnp.sum(jnp.where(ids == expert, gates, 0.0), axis=1, keepdims=True))

    for j in range(j_steps):
        cols = slice(j * out_chunk, (j + 1) * out_chunk)
        wait_for(yr.at[j], y_recv.at[j])
        total = residual[:, cols]
        for expert in range(EXPERTS):
            share = None
            for group in range(groups):
                for i in range(per_expert):
                    term = yr[j, group * per_group + expert * per_expert + i].astype(jnp.float32)
                    share = term if share is None else share + term
            total = total + weights[expert] * share
        out_ref[:, cols] = total.astype(out_ref.dtype)

    @pl.loop(0, k_steps)
    def _(k):
        wait_for(xd.at[k], x_send.at[k])
        forward(k).wait_send()

    @pl.loop(0, j_steps)
    def _(j):
        give(j).wait_send()
        wait_for(ys.at[j], y_send.at[j])


def shared_local(
    residual_in,
    queries,
    fresh_keys,
    fresh_values,
    stored_keys,
    stored_values,
    context_len,
    norm_gain,
    expert_ids,
    expert_gates,
    gate_weight,
    up_weight,
    down_weight,
):
    groups, n = lax.axis_size("groups"), lax.axis_size("ep")
    reqs, features = residual_in.shape
    units = gate_weight.shape[1] // groups
    chips = groups * n // 2
    rows = chips * reqs
    k_steps, j_steps = features // IN_CHUNK, features // OUT_CHUNK
    bf16, f32 = jnp.bfloat16, jnp.float32
    vmem = pl.BlockSpec(memory_space=pltpu.VMEM)
    hbm = pl.BlockSpec(memory_space=pl.ANY)
    dma = pltpu.SemaphoreType.DMA
    return pl.pallas_call(
        functools.partial(shared_kernel, groups, n),
        out_shape=jax.ShapeDtypeStruct((reqs, features), bf16),
        in_specs=[hbm] * 13,
        out_specs=vmem,
        scratch_shapes=[
            pltpu.SMEM(context_len.shape, jnp.int32),
            pltpu.VMEM((reqs, features), bf16),
            pltpu.VMEM((reqs, features), bf16),
            pltpu.VMEM(fresh_keys.shape, bf16),
            pltpu.VMEM(fresh_values.shape, bf16),
            pltpu.VMEM((1, features), f32),
            pltpu.VMEM(expert_ids.shape, jnp.int32),
            pltpu.VMEM(expert_gates.shape, bf16),
            pltpu.VMEM(stored_keys.shape, bf16),
            pltpu.VMEM(stored_values.shape, bf16),
            pltpu.VMEM((k_steps, IN_CHUNK, units), bf16),
            pltpu.VMEM((k_steps, IN_CHUNK, units), bf16),
            pltpu.VMEM((j_steps, units, OUT_CHUNK), bf16),
            pltpu.VMEM((reqs * features // HEAD_WIDTH, HEAD_WIDTH), f32),
            pltpu.VMEM((reqs, features), f32),
            pltpu.VMEM((k_steps, reqs, IN_CHUNK), bf16),
            pltpu.VMEM((k_steps, chips, reqs, IN_CHUNK), bf16),
            pltpu.VMEM((k_steps, chips, reqs, IN_CHUNK), bf16),
            pltpu.VMEM((2 * rows, IN_CHUNK), f32),
            pltpu.VMEM((2 * rows, units), f32),
            pltpu.VMEM((2 * rows, units), f32),
            pltpu.VMEM((2 * rows, units), bf16),
            pltpu.VMEM((j_steps, rows, OUT_CHUNK), f32),
            pltpu.VMEM((j_steps, rows, OUT_CHUNK), bf16),
            pltpu.VMEM((j_steps, rows, OUT_CHUNK), bf16),
            pltpu.VMEM((j_steps, chips, reqs, OUT_CHUNK), bf16),
            pltpu.VMEM((j_steps, chips, reqs, OUT_CHUNK), bf16),
            dma((10,)),
            dma((k_steps,)),
            dma((k_steps,)),
            dma((j_steps,)),
            dma((k_steps,)),
            dma((k_steps,)),
            dma((k_steps,)),
            dma((k_steps,)),
            dma((j_steps,)),
            dma((j_steps,)),
            dma((j_steps,)),
            dma((j_steps,)),
        ],
        compiler_params=pltpu.CompilerParams(
            collective_id=0, has_side_effects=True, vmem_limit_bytes=66_000_000
        ),
        name="decode_step",
    )(
        context_len,
        residual_in,
        queries,
        fresh_keys,
        fresh_values,
        norm_gain.reshape(1, features),
        expert_ids,
        expert_gates,
        stored_keys,
        stored_values,
        gate_weight,
        up_weight,
        down_weight,
    )


def kernel(
    n,
    *refs,
):
    small_hbm, refs = refs[:10], refs[10:]
    small, refs = refs[4:14], refs[:4] + refs[14:]
    (
    wg_hbm,
    wu_hbm,
    wd_hbm,
    out_ref,
    wg,
    wu,
    wd,
    q_rows,
    residual,
    xr,
    x32,
    acc_g,
    acc_u,
    hidden,
    ys,
    yr,
    in_sem,
    g_sem,
    u_sem,
    d_sem,
    x_send,
    x_recv,
    y_send,
    y_recv,
    ) = refs
    ctx_ref, res_ref, q_ref, fk_ref, fv_ref, gain_ref, ids_ref, gates_ref, k_buf, v_buf = small
    me = lax.axis_index("ep")
    split = n // EXPERTS
    reqs, features = res_ref.shape
    k_steps = features // CHUNK
    ring = wg.shape[0]

    loads = [
        pltpu.make_async_copy(source, target, in_sem.at[i])
        for i, (source, target) in enumerate(zip(small_hbm, small))
    ]
    for load in loads:
        load.start()

    def gate_copy(step, slot):
        rows = pl.ds(pl.multiple_of(step * CHUNK, CHUNK), CHUNK)
        return pltpu.make_async_copy(wg_hbm.at[rows, :], wg.at[slot], g_sem.at[slot])

    def up_copy(step, slot):
        rows = pl.ds(pl.multiple_of(step * CHUNK, CHUNK), CHUNK)
        return pltpu.make_async_copy(wu_hbm.at[rows, :], wu.at[slot], u_sem.at[slot])

    def down_copy(step):
        cols = pl.ds(pl.multiple_of(step * CHUNK, CHUNK), CHUNK)
        return pltpu.make_async_copy(wd_hbm.at[:, cols], wd.at[step], d_sem.at[step])

    early = min(EARLY, k_steps)
    for step in range(ring):
        gate_copy(step, step).start(priority=1)
        up_copy(step, step).start(priority=1)
    for step in range(early):
        down_copy(step).start(priority=1)

    barrier = pltpu.get_barrier_semaphore()

    @pl.loop(1, n)
    def _(d):
        pl.semaphore_signal(
            barrier, inc=1, device_id={"ep": lax.rem(me + d, n)}, device_id_type=MESH
        )

    acc_g[...] = jnp.zeros_like(acc_g)
    acc_u[...] = jnp.zeros_like(acc_u)
    for load in loads:
        load.wait()
    attend(q_ref, fk_ref, fv_ref, k_buf, v_buf, ctx_ref, q_rows, residual)
    full = res_ref[...].astype(jnp.float32) + residual[...]
    residual[...] = full
    factor = lax.rsqrt(jnp.mean(full * full, axis=1, keepdims=True) + norm_eps)
    normed = (full * factor * gain_ref[...]).astype(jnp.bfloat16)
    for k in range(k_steps):
        xr[k, 0] = normed[:, k * CHUNK : (k + 1) * CHUNK]

    pl.semaphore_wait(barrier, n - 1)

    ahead = k_steps

    def send_rows(k):
        @pl.loop(1, n)
        def _(d):
            pltpu.make_async_remote_copy(
                src_ref=xr.at[k, 0],
                dst_ref=xr.at[k, d],
                send_sem=x_send.at[k],
                recv_sem=x_recv.at[k],
                device_id={"ep": lax.rem(me + d, n)},
                device_id_type=MESH,
            ).start()

    for k in range(ahead):
        send_rows(k)

    def wait_blocks(ref, sem):
        pltpu.make_async_copy(ref, ref, sem).wait()

    @pl.loop(0, k_steps)
    def _(k):
        slot = lax.rem(k, ring)

        @pl.when(k + ahead < k_steps)
        def _():
            send_rows(k + ahead)

        wait_blocks(xr.at[k, pl.ds(1, n - 1)], x_recv.at[k])
        for d in range(n):
            x32[reqs * d : reqs * (d + 1), :] = xr[k, d].astype(jnp.float32)
        x = x32[...].astype(jnp.bfloat16)
        gate_copy(k, slot).wait()
        acc_g[...] += jnp.dot(x, wg[slot], preferred_element_type=jnp.float32)
        up_copy(k, slot).wait()
        acc_u[...] += jnp.dot(x, wu[slot], preferred_element_type=jnp.float32)

        @pl.when(k + ring < k_steps)
        def _():
            gate_copy(k + ring, slot).start(priority=1)
            up_copy(k + ring, slot).start(priority=1)

        @pl.when(k == max(k_steps - ring - 1, 0))
        def _():
            @pl.loop(early, k_steps)
            def _(j):
                down_copy(j).start(priority=1)

    gate = acc_g[...]
    hidden[...] = (gate / (1.0 + jnp.exp(-gate)) * acc_u[...]).astype(jnp.bfloat16)

    @pl.loop(0, k_steps)
    def _(j):
        down_copy(j).wait()
        part = jnp.dot(hidden[...], wd[j], preferred_element_type=jnp.float32)
        yr[j, 0] = part[0:reqs].astype(jnp.bfloat16)
        for d in range(1, n):
            ys[j, d] = part[reqs * d : reqs * (d + 1)].astype(jnp.bfloat16)

        @pl.loop(1, n)
        def _(d):
            pltpu.make_async_remote_copy(
                src_ref=ys.at[j, d],
                dst_ref=yr.at[j, d],
                send_sem=y_send.at[j],
                recv_sem=y_recv.at[j],
                device_id={"ep": lax.rem(me - d + n, n)},
                device_id_type=MESH,
            ).start()

    ids = ids_ref[...]
    gates = gates_ref[...].astype(jnp.float32)
    weights = []
    for expert in range(EXPERTS):
        weights.append(jnp.sum(jnp.where(ids == expert, gates, 0.0), axis=1, keepdims=True))

    for j in range(k_steps):
        cols = slice(j * CHUNK, (j + 1) * CHUNK)
        wait_blocks(yr.at[j, pl.ds(1, n - 1)], y_recv.at[j])
        total = residual[:, cols]
        for d in range(n):
            expert = lax.rem(me + d, n) // split
            weight = weights[0]
            for other in range(1, EXPERTS):
                weight = jnp.where(expert == other, weights[other], weight)
            total = total + weight * yr[j, d].astype(jnp.float32)
        out_ref[:, cols] = total.astype(out_ref.dtype)

    @pl.loop(0, k_steps)
    def _(k):
        wait_blocks(xr.at[k, pl.ds(1, n - 1)], x_send.at[k])
        wait_blocks(ys.at[k, pl.ds(1, n - 1)], y_send.at[k])


def plain_local(
    residual_in,
    queries,
    fresh_keys,
    fresh_values,
    stored_keys,
    stored_values,
    context_len,
    norm_gain,
    expert_ids,
    expert_gates,
    gate_weight,
    up_weight,
    down_weight,
):
    n = lax.axis_size("ep")
    reqs, features = residual_in.shape
    units = gate_weight.shape[1]
    steps = features // CHUNK
    ring = min(RING, steps)
    bf16, f32 = jnp.bfloat16, jnp.float32
    vmem = pl.BlockSpec(memory_space=pltpu.VMEM)
    hbm = pl.BlockSpec(memory_space=pl.ANY)
    dma = pltpu.SemaphoreType.DMA
    rows = n * reqs
    return pl.pallas_call(
        functools.partial(kernel, n),
        out_shape=jax.ShapeDtypeStruct((reqs, features), bf16),
        in_specs=[hbm] * 13,
        out_specs=vmem,
        scratch_shapes=[
            pltpu.SMEM(context_len.shape, jnp.int32),
            pltpu.VMEM((reqs, features), bf16),
            pltpu.VMEM((reqs, features), bf16),
            pltpu.VMEM(fresh_keys.shape, bf16),
            pltpu.VMEM(fresh_values.shape, bf16),
            pltpu.VMEM((1, features), f32),
            pltpu.VMEM(expert_ids.shape, jnp.int32),
            pltpu.VMEM(expert_gates.shape, bf16),
            pltpu.VMEM(stored_keys.shape, bf16),
            pltpu.VMEM(stored_values.shape, bf16),
            pltpu.VMEM((ring, CHUNK, units), bf16),
            pltpu.VMEM((ring, CHUNK, units), bf16),
            pltpu.VMEM((steps, units, CHUNK), bf16),
            pltpu.VMEM((reqs * features // HEAD_WIDTH, HEAD_WIDTH), f32),
            pltpu.VMEM((reqs, features), f32),
            pltpu.VMEM((steps, n, reqs, CHUNK), bf16),
            pltpu.VMEM((rows, CHUNK), f32),
            pltpu.VMEM((rows, units), f32),
            pltpu.VMEM((rows, units), f32),
            pltpu.VMEM((rows, units), bf16),
            pltpu.VMEM((steps, n, reqs, CHUNK), bf16),
            pltpu.VMEM((steps, n, reqs, CHUNK), bf16),
            dma((10,)),
            dma((ring,)),
            dma((ring,)),
            dma((steps,)),
            dma((steps,)),
            dma((steps,)),
            dma((steps,)),
            dma((steps,)),
        ],
        compiler_params=pltpu.CompilerParams(
            collective_id=0, has_side_effects=True, vmem_limit_bytes=66_000_000
        ),
        name="decode_step",
    )(
        context_len,
        residual_in,
        queries,
        fresh_keys,
        fresh_values,
        norm_gain.reshape(1, features),
        expert_ids,
        expert_gates,
        stored_keys,
        stored_values,
        gate_weight,
        up_weight,
        down_weight,
    )


def solution(mesh):
    in_specs = (
        P(("groups", "ep"), None),
        P(("groups", "ep"), None),
        P(("groups", "ep"), None),
        P(("groups", "ep"), None),
        P(("groups", "ep"), None, None),
        P(("groups", "ep"), None, None),
        P(("groups", "ep")),
        P(),
        P(("groups", "ep"), None),
        P(("groups", "ep"), None),
        P(None, "ep"),
        P(None, "ep"),
        P("ep", None),
    )
    out_specs = P(("groups", "ep"), None)
    groups, n = mesh.shape["groups"], mesh.shape["ep"]

    def local(*args):
        units = args[10].shape[1]
        shared = n % (2 * EXPERTS) == 0 and units % (128 * groups) == 0
        return (shared_local if shared else plain_local)(*args)

    return jax.shard_map(local, mesh=mesh, in_specs=in_specs, out_specs=out_specs, check_vma=False)
```

```python
import functools
import math

import jax
import jax.numpy as jnp
from jax import lax
from jax.experimental import pallas as pl
from jax.experimental.pallas import tpu as pltpu
from jax.sharding import PartitionSpec as P

KEY_VALUE_HEADS = 4
HEAD_WIDTH = 128
EXPERTS = 4
CHUNK = 512
RING = 5
EARLY = 3
IN_CHUNK = 1024
OUT_CHUNK = 1024
LAG = 1
SHARED_VMEM = 66_000_000

norm_eps = 1e-05
MESH = pl.DeviceIdType.MESH


def attend(q_ref, fk_ref, fv_ref, k_ref, v_ref, ctx_ref, q_rows, att):
    reqs, features = q_ref.shape
    positions = k_ref.shape[1]
    heads = features // HEAD_WIDTH
    group = heads // KEY_VALUE_HEADS
    scale = 1.0 / math.sqrt(HEAD_WIDTH)
    q = q_ref[...].astype(jnp.float32)
    fk = fk_ref[...].astype(jnp.float32)
    fv = fv_ref[...].astype(jnp.float32)
    for r in range(reqs):
        for h in range(heads):
            q_rows[r * heads + h : r * heads + h + 1, :] = q[
                r : r + 1, h * HEAD_WIDTH : (h + 1) * HEAD_WIDTH
            ]
    scores, own, valid = [], [], []
    position = lax.broadcasted_iota(jnp.int32, (heads, positions), 1)
    for r in range(reqs):
        valid.append(position < ctx_ref[r])
        for j in range(KEY_VALUE_HEADS):
            rows = slice(r * heads + j * group, r * heads + (j + 1) * group)
            cols = slice(j * HEAD_WIDTH, (j + 1) * HEAD_WIDTH)
            qj = q_rows[rows, :]
            scores.append(
                lax.dot_general(
                    qj.astype(jnp.bfloat16),
                    k_ref[r, :, cols],
                    (((1,), (1,)), ((), ())),
                    preferred_element_type=jnp.float32,
                )
            )
            own.append(jnp.sum(qj * fk[r : r + 1, cols], axis=1, keepdims=True))
    ok = jnp.concatenate(valid, axis=0)
    s = jnp.concatenate(scores, axis=0) * scale
    o = jnp.concatenate(own, axis=0) * scale
    m = jnp.maximum(jnp.max(jnp.where(ok, s, -1e30), axis=1, keepdims=True), o)
    e = jnp.where(ok, jnp.exp(s - m), 0.0)
    oe = jnp.exp(o - m)
    total = jnp.sum(e, axis=1, keepdims=True) + oe
    w = (e / total).astype(jnp.bfloat16)
    ow = (oe / total).astype(jnp.bfloat16).astype(jnp.float32)
    for r in range(reqs):
        for j in range(KEY_VALUE_HEADS):
            rows = slice(r * heads + j * group, r * heads + (j + 1) * group)
            cols = slice(j * HEAD_WIDTH, (j + 1) * HEAD_WIDTH)
            mixed = jnp.dot(w[rows], v_ref[r, :, cols], preferred_element_type=jnp.float32)
            mixed = mixed + ow[rows] * fv[r : r + 1, cols]
            for g in range(group):
                h = j * group + g
                att[r : r + 1, h * HEAD_WIDTH : (h + 1) * HEAD_WIDTH] = mixed[g : g + 1, :]


def shared_kernel(groups, n, *refs):
    small_hbm, refs = refs[:10], refs[10:]
    small, refs = refs[4:14], refs[:4] + refs[14:]
    (
        wg_hbm,
        wu_hbm,
        wd_hbm,
        out_ref,
        wg,
        wu,
        wd,
        q_rows,
        residual,
        xs,
        xd,
        xf,
        x32s,
        acc_g,
        acc_u,
        hidden,
        keep,
        ps,
        pr,
        ys,
        yr,
        in_sem,
        w_sem,
        x_send,
        x_recv,
        f_send,
        f_recv,
        p_send,
        p_recv,
        y_send,
        y_recv,
    ) = refs
    ctx_ref, res_ref, q_ref, fk_ref, fv_ref, gain_ref, ids_ref, gates_ref, k_buf, v_buf = small
    g, e = lax.axis_index("groups"), lax.axis_index("ep")
    per_group = n // 2
    chips = groups * per_group
    core = lax.rem(e, 2)
    chip = g * per_group + e // 2
    partner = {"groups": g, "ep": e + 1 - 2 * core}
    reqs, features = res_ref.shape
    k_steps, chunk, units = wg.shape
    j_steps, _, out_chunk = wd.shape
    rows = chips * reqs

    place = e // 2

    def turned(at, by, size):
        moved = at + by
        return moved - jnp.where(moved >= size, size, 0)

    targets = []
    near = sorted(range(per_group), key=lambda t: abs(t - per_group // 2))
    for t in near:
        for s in reversed(range(groups)):
            to_group, to_place = turned(g, s, groups), turned(place, t, per_group)
            targets.append(
                (
                    to_group * per_group + to_place,
                    {"groups": to_group, "ep": to_place * 2 + 1 - core},
                )
            )

    barrier = pltpu.get_barrier_semaphore()
    for _, device in targets:
        pl.semaphore_signal(barrier, inc=1, device_id=device, device_id_type=MESH)

    loads = [
        pltpu.make_async_copy(source, target, in_sem.at[i])
        for i, (source, target) in enumerate(zip(small_hbm, small))
    ]
    for load in loads:
        load.start()

    first = pl.multiple_of(g * units, 128)

    def gate_copy(step):
        at = pl.ds(pl.multiple_of(step * chunk, chunk), chunk)
        return pltpu.make_async_copy(wg_hbm.at[at, pl.ds(first, units)], wg.at[step], w_sem.at[0])

    def up_copy(step):
        at = pl.ds(pl.multiple_of(step * chunk, chunk), chunk)
        return pltpu.make_async_copy(wu_hbm.at[at, pl.ds(first, units)], wu.at[step], w_sem.at[1])

    def down_copy(step):
        at = pl.ds(pl.multiple_of(step * out_chunk, out_chunk), out_chunk)
        return pltpu.make_async_copy(wd_hbm.at[pl.ds(first, units), at], wd.at[step], w_sem.at[2])

    @pl.loop(0, k_steps)
    def _(step):
        gate_copy(step).start(priority=1)
        up_copy(step).start(priority=1)

    @pl.loop(0, j_steps)
    def _(step):
        down_copy(step).start(priority=1)

    acc_g[...] = jnp.zeros_like(acc_g)
    acc_u[...] = jnp.zeros_like(acc_u)
    for load in loads:
        load.wait()
    attend(q_ref, fk_ref, fv_ref, k_buf, v_buf, ctx_ref, q_rows, residual)
    full = res_ref[...].astype(jnp.float32) + residual[...]
    residual[...] = full
    factor = lax.rsqrt(jnp.mean(full * full, axis=1, keepdims=True) + norm_eps)
    normed = (full * factor * gain_ref[...]).astype(jnp.bfloat16)
    for k in range(k_steps):
        xs[k] = normed[:, k * chunk : (k + 1) * chunk]

    pl.semaphore_wait(barrier, chips)

    @pl.loop(0, k_steps)
    def _(k):
        for _, device in targets:
            pltpu.make_async_remote_copy(
                src_ref=xs.at[k],
                dst_ref=xd.at[k, chip],
                send_sem=x_send.at[0],
                recv_sem=x_recv.at[k],
                device_id=device,
                device_id_type=MESH,
            ).start()

    def wait_for(ref, sem):
        pltpu.make_async_copy(ref, ref, sem).wait()

    def forward(k):
        return pltpu.make_async_remote_copy(
            src_ref=xd.at[k],
            dst_ref=xf.at[k],
            send_sem=f_send.at[0],
            recv_sem=f_recv.at[k],
            device_id=partner,
            device_id_type=MESH,
        )

    def pass_on(k):
        wait_for(xd.at[k], x_recv.at[k])
        forward(k).start()

    pass_on(0)
    for k in range(k_steps):
        if k + 1 < k_steps:
            pass_on(k + 1)
        forward(k).wait_recv()
        x32 = x32s.at[k % 2]
        for q in range(chips):
            x32[reqs * q : reqs * (q + 1), :] = xd[k, q].astype(jnp.float32)
            x32[rows + reqs * q : rows + reqs * (q + 1), :] = xf[k, q].astype(jnp.float32)
        x = x32[...].astype(jnp.bfloat16)
        if k == 0:
            wait_for(wg, w_sem.at[0])
            wait_for(wu, w_sem.at[1])
        acc_g[...] += jnp.dot(x, wg[k], preferred_element_type=jnp.float32)
        acc_u[...] += jnp.dot(x, wu[k], preferred_element_type=jnp.float32)

    gate = acc_g[...]
    hidden[...] = (gate / (1.0 + jnp.exp(-gate)) * acc_u[...]).astype(jnp.bfloat16)

    def give(j):
        return pltpu.make_async_remote_copy(
            src_ref=ps.at[j],
            dst_ref=pr.at[j],
            send_sem=p_send.at[0],
            recv_sem=p_recv.at[j],
            device_id=partner,
            device_id_type=MESH,
        )

    def send_back(j):
        give(j).wait_recv()
        both = (keep[j] + pr[j].astype(jnp.float32)).astype(jnp.bfloat16)
        for q in range(chips):
            ys[j, q] = both[reqs * q : reqs * (q + 1)]

        for q, device in targets:
            pltpu.make_async_remote_copy(
                src_ref=ys.at[j, q],
                dst_ref=yr.at[j, chip],
                send_sem=y_send.at[0],
                recv_sem=y_recv.at[j],
                device_id=device,
                device_id_type=MESH,
            ).start()

    wait_for(wd, w_sem.at[2])
    for j in range(j_steps + LAG):
        if j < j_steps:
            part = jnp.dot(hidden[...], wd[j], preferred_element_type=jnp.float32)
            keep[j] = part[0:rows]
            ps[j] = part[rows:].astype(jnp.bfloat16)
            give(j).start()
        if j >= LAG:
            send_back(j - LAG)

    ids = ids_ref[...]
    gates = gates_ref[...].astype(jnp.float32)
    per_expert = per_group // EXPERTS
    weights = []
    for expert in range(EXPERTS):
        weights.append(jnp.sum(jnp.where(ids == expert, gates, 0.0), axis=1, keepdims=True))

    for j in range(j_steps):
        cols = slice(j * out_chunk, (j + 1) * out_chunk)
        wait_for(yr.at[j], y_recv.at[j])
        total = residual[:, cols]
        for expert in range(EXPERTS):
            share = None
            for group in range(groups):
                for i in range(per_expert):
                    term = yr[j, group * per_group + expert * per_expert + i].astype(jnp.float32)
                    share = term if share is None else share + term
            total = total + weights[expert] * share
        out_ref[:, cols] = total.astype(out_ref.dtype)

    wait_for(xd, x_send.at[0])
    wait_for(xd, f_send.at[0])
    wait_for(ps, p_send.at[0])
    wait_for(ys, y_send.at[0])


def shared_local(
    residual_in,
    queries,
    fresh_keys,
    fresh_values,
    stored_keys,
    stored_values,
    context_len,
    norm_gain,
    expert_ids,
    expert_gates,
    gate_weight,
    up_weight,
    down_weight,
):
    groups, n = lax.axis_size("groups"), lax.axis_size("ep")
    reqs, features = residual_in.shape
    units = gate_weight.shape[1] // groups
    chips = groups * n // 2
    rows = chips * reqs
    k_steps, j_steps = features // IN_CHUNK, features // OUT_CHUNK
    bf16, f32 = jnp.bfloat16, jnp.float32
    vmem = pl.BlockSpec(memory_space=pltpu.VMEM)
    hbm = pl.BlockSpec(memory_space=pltpu.HBM)
    dma = pltpu.SemaphoreType.DMA
    return pl.pallas_call(
        functools.partial(shared_kernel, groups, n),
        out_shape=jax.ShapeDtypeStruct((reqs, features), bf16),
        in_specs=[hbm] * 13,
        out_specs=vmem,
        scratch_shapes=[
            pltpu.SMEM(context_len.shape, jnp.int32),
            pltpu.VMEM((reqs, features), bf16),
            pltpu.VMEM((reqs, features), bf16),
            pltpu.VMEM(fresh_keys.shape, bf16),
            pltpu.VMEM(fresh_values.shape, bf16),
            pltpu.VMEM((1, features), f32),
            pltpu.VMEM(expert_ids.shape, jnp.int32),
            pltpu.VMEM(expert_gates.shape, bf16),
            pltpu.VMEM(stored_keys.shape, bf16),
            pltpu.VMEM(stored_values.shape, bf16),
            pltpu.VMEM((k_steps, IN_CHUNK, units), bf16),
            pltpu.VMEM((k_steps, IN_CHUNK, units), bf16),
            pltpu.VMEM((j_steps, units, OUT_CHUNK), bf16),
            pltpu.VMEM((reqs * features // HEAD_WIDTH, HEAD_WIDTH), f32),
            pltpu.VMEM((reqs, features), f32),
            pltpu.VMEM((k_steps, reqs, IN_CHUNK), bf16),
            pltpu.VMEM((k_steps, chips, reqs, IN_CHUNK), bf16),
            pltpu.VMEM((k_steps, chips, reqs, IN_CHUNK), bf16),
            pltpu.VMEM((2, 2 * rows, IN_CHUNK), f32),
            pltpu.VMEM((2 * rows, units), f32),
            pltpu.VMEM((2 * rows, units), f32),
            pltpu.VMEM((2 * rows, units), bf16),
            pltpu.VMEM((j_steps, rows, OUT_CHUNK), f32),
            pltpu.VMEM((j_steps, rows, OUT_CHUNK), bf16),
            pltpu.VMEM((j_steps, rows, OUT_CHUNK), bf16),
            pltpu.VMEM((j_steps, chips, reqs, OUT_CHUNK), bf16),
            pltpu.VMEM((j_steps, chips, reqs, OUT_CHUNK), bf16),
            dma((10,)),
            dma((3,)),
            dma((1,)),
            dma((k_steps,)),
            dma((1,)),
            dma((k_steps,)),
            dma((1,)),
            dma((j_steps,)),
            dma((1,)),
            dma((j_steps,)),
        ],
        compiler_params=pltpu.CompilerParams(
            collective_id=0, has_side_effects=True, vmem_limit_bytes=SHARED_VMEM
        ),
        name="decode_step",
    )(
        context_len,
        residual_in,
        queries,
        fresh_keys,
        fresh_values,
        norm_gain.reshape(1, features),
        expert_ids,
        expert_gates,
        stored_keys,
        stored_values,
        gate_weight,
        up_weight,
        down_weight,
    )


def kernel(
    n,
    *refs,
):
    small_hbm, refs = refs[:10], refs[10:]
    small, refs = refs[4:14], refs[:4] + refs[14:]
    (
    wg_hbm,
    wu_hbm,
    wd_hbm,
    out_ref,
    wg,
    wu,
    wd,
    q_rows,
    residual,
    xr,
    x32,
    acc_g,
    acc_u,
    hidden,
    ys,
    yr,
    in_sem,
    g_sem,
    u_sem,
    d_sem,
    x_send,
    x_recv,
    y_send,
    y_recv,
    ) = refs
    ctx_ref, res_ref, q_ref, fk_ref, fv_ref, gain_ref, ids_ref, gates_ref, k_buf, v_buf = small
    me = lax.axis_index("ep")
    split = n // EXPERTS
    reqs, features = res_ref.shape
    k_steps = features // CHUNK
    ring = wg.shape[0]

    loads = [
        pltpu.make_async_copy(source, target, in_sem.at[i])
        for i, (source, target) in enumerate(zip(small_hbm, small))
    ]
    for load in loads:
        load.start()

    def gate_copy(step, slot):
        rows = pl.ds(pl.multiple_of(step * CHUNK, CHUNK), CHUNK)
        return pltpu.make_async_copy(wg_hbm.at[rows, :], wg.at[slot], g_sem.at[slot])

    def up_copy(step, slot):
        rows = pl.ds(pl.multiple_of(step * CHUNK, CHUNK), CHUNK)
        return pltpu.make_async_copy(wu_hbm.at[rows, :], wu.at[slot], u_sem.at[slot])

    def down_copy(step):
        cols = pl.ds(pl.multiple_of(step * CHUNK, CHUNK), CHUNK)
        return pltpu.make_async_copy(wd_hbm.at[:, cols], wd.at[step], d_sem.at[step])

    early = min(EARLY, k_steps)
    for step in range(ring):
        gate_copy(step, step).start(priority=1)
        up_copy(step, step).start(priority=1)
    for step in range(early):
        down_copy(step).start(priority=1)

    barrier = pltpu.get_barrier_semaphore()

    @pl.loop(1, n)
    def _(d):
        pl.semaphore_signal(
            barrier, inc=1, device_id={"ep": lax.rem(me + d, n)}, device_id_type=MESH
        )

    acc_g[...] = jnp.zeros_like(acc_g)
    acc_u[...] = jnp.zeros_like(acc_u)
    for load in loads:
        load.wait()
    attend(q_ref, fk_ref, fv_ref, k_buf, v_buf, ctx_ref, q_rows, residual)
    full = res_ref[...].astype(jnp.float32) + residual[...]
    residual[...] = full
    factor = lax.rsqrt(jnp.mean(full * full, axis=1, keepdims=True) + norm_eps)
    normed = (full * factor * gain_ref[...]).astype(jnp.bfloat16)
    for k in range(k_steps):
        xr[k, 0] = normed[:, k * CHUNK : (k + 1) * CHUNK]

    pl.semaphore_wait(barrier, n - 1)

    ahead = k_steps

    def send_rows(k):
        @pl.loop(1, n)
        def _(d):
            pltpu.make_async_remote_copy(
                src_ref=xr.at[k, 0],
                dst_ref=xr.at[k, d],
                send_sem=x_send.at[k],
                recv_sem=x_recv.at[k],
                device_id={"ep": lax.rem(me + d, n)},
                device_id_type=MESH,
            ).start()

    for k in range(ahead):
        send_rows(k)

    def wait_blocks(ref, sem):
        pltpu.make_async_copy(ref, ref, sem).wait()

    @pl.loop(0, k_steps)
    def _(k):
        slot = lax.rem(k, ring)

        @pl.when(k + ahead < k_steps)
        def _():
            send_rows(k + ahead)

        wait_blocks(xr.at[k, pl.ds(1, n - 1)], x_recv.at[k])
        for d in range(n):
            x32[reqs * d : reqs * (d + 1), :] = xr[k, d].astype(jnp.float32)
        x = x32[...].astype(jnp.bfloat16)
        gate_copy(k, slot).wait()
        acc_g[...] += jnp.dot(x, wg[slot], preferred_element_type=jnp.float32)
        up_copy(k, slot).wait()
        acc_u[...] += jnp.dot(x, wu[slot], preferred_element_type=jnp.float32)

        @pl.when(k + ring < k_steps)
        def _():
            gate_copy(k + ring, slot).start(priority=1)
            up_copy(k + ring, slot).start(priority=1)

        @pl.when(k == max(k_steps - ring - 1, 0))
        def _():
            @pl.loop(early, k_steps)
            def _(j):
                down_copy(j).start(priority=1)

    gate = acc_g[...]
    hidden[...] = (gate / (1.0 + jnp.exp(-gate)) * acc_u[...]).astype(jnp.bfloat16)

    @pl.loop(0, k_steps)
    def _(j):
        down_copy(j).wait()
        part = jnp.dot(hidden[...], wd[j], preferred_element_type=jnp.float32)
        yr[j, 0] = part[0:reqs].astype(jnp.bfloat16)
        for d in range(1, n):
            ys[j, d] = part[reqs * d : reqs * (d + 1)].astype(jnp.bfloat16)

        @pl.loop(1, n)
        def _(d):
            pltpu.make_async_remote_copy(
                src_ref=ys.at[j, d],
                dst_ref=yr.at[j, d],
                send_sem=y_send.at[j],
                recv_sem=y_recv.at[j],
                device_id={"ep": lax.rem(me - d + n, n)},
                device_id_type=MESH,
            ).start()

    ids = ids_ref[...]
    gates = gates_ref[...].astype(jnp.float32)
    weights = []
    for expert in range(EXPERTS):
        weights.append(jnp.sum(jnp.where(ids == expert, gates, 0.0), axis=1, keepdims=True))

    for j in range(k_steps):
        cols = slice(j * CHUNK, (j + 1) * CHUNK)
        wait_blocks(yr.at[j, pl.ds(1, n - 1)], y_recv.at[j])
        total = residual[:, cols]
        for d in range(n):
            expert = lax.rem(me + d, n) // split
            weight = weights[0]
            for other in range(1, EXPERTS):
                weight = jnp.where(expert == other, weights[other], weight)
            total = total + weight * yr[j, d].astype(jnp.float32)
        out_ref[:, cols] = total.astype(out_ref.dtype)

    @pl.loop(0, k_steps)
    def _(k):
        wait_blocks(xr.at[k, pl.ds(1, n - 1)], x_send.at[k])
        wait_blocks(ys.at[k, pl.ds(1, n - 1)], y_send.at[k])


def plain_local(
    residual_in,
    queries,
    fresh_keys,
    fresh_values,
    stored_keys,
    stored_values,
    context_len,
    norm_gain,
    expert_ids,
    expert_gates,
    gate_weight,
    up_weight,
    down_weight,
):
    n = lax.axis_size("ep")
    reqs, features = residual_in.shape
    units = gate_weight.shape[1]
    steps = features // CHUNK
    ring = min(RING, steps)
    bf16, f32 = jnp.bfloat16, jnp.float32
    vmem = pl.BlockSpec(memory_space=pltpu.VMEM)
    hbm = pl.BlockSpec(memory_space=pl.ANY)
    dma = pltpu.SemaphoreType.DMA
    rows = n * reqs
    return pl.pallas_call(
        functools.partial(kernel, n),
        out_shape=jax.ShapeDtypeStruct((reqs, features), bf16),
        in_specs=[hbm] * 13,
        out_specs=vmem,
        scratch_shapes=[
            pltpu.SMEM(context_len.shape, jnp.int32),
            pltpu.VMEM((reqs, features), bf16),
            pltpu.VMEM((reqs, features), bf16),
            pltpu.VMEM(fresh_keys.shape, bf16),
            pltpu.VMEM(fresh_values.shape, bf16),
            pltpu.VMEM((1, features), f32),
            pltpu.VMEM(expert_ids.shape, jnp.int32),
            pltpu.VMEM(expert_gates.shape, bf16),
            pltpu.VMEM(stored_keys.shape, bf16),
            pltpu.VMEM(stored_values.shape, bf16),
            pltpu.VMEM((ring, CHUNK, units), bf16),
            pltpu.VMEM((ring, CHUNK, units), bf16),
            pltpu.VMEM((steps, units, CHUNK), bf16),
            pltpu.VMEM((reqs * features // HEAD_WIDTH, HEAD_WIDTH), f32),
            pltpu.VMEM((reqs, features), f32),
            pltpu.VMEM((steps, n, reqs, CHUNK), bf16),
            pltpu.VMEM((rows, CHUNK), f32),
            pltpu.VMEM((rows, units), f32),
            pltpu.VMEM((rows, units), f32),
            pltpu.VMEM((rows, units), bf16),
            pltpu.VMEM((steps, n, reqs, CHUNK), bf16),
            pltpu.VMEM((steps, n, reqs, CHUNK), bf16),
            dma((10,)),
            dma((ring,)),
            dma((ring,)),
            dma((steps,)),
            dma((steps,)),
            dma((steps,)),
            dma((steps,)),
            dma((steps,)),
        ],
        compiler_params=pltpu.CompilerParams(
            collective_id=0, has_side_effects=True, vmem_limit_bytes=66_000_000
        ),
        name="decode_step",
    )(
        context_len,
        residual_in,
        queries,
        fresh_keys,
        fresh_values,
        norm_gain.reshape(1, features),
        expert_ids,
        expert_gates,
        stored_keys,
        stored_values,
        gate_weight,
        up_weight,
        down_weight,
    )


def solution(mesh):
    in_specs = (
        P(("groups", "ep"), None),
        P(("groups", "ep"), None),
        P(("groups", "ep"), None),
        P(("groups", "ep"), None),
        P(("groups", "ep"), None, None),
        P(("groups", "ep"), None, None),
        P(("groups", "ep")),
        P(),
        P(("groups", "ep"), None),
        P(("groups", "ep"), None),
        P(None, "ep"),
        P(None, "ep"),
        P("ep", None),
    )
    out_specs = P(("groups", "ep"), None)
    groups, n = mesh.shape["groups"], mesh.shape["ep"]

    def local(*args):
        units = args[10].shape[1]
        shared = n % (2 * EXPERTS) == 0 and units % (128 * groups) == 0
        return (shared_local if shared else plain_local)(*args)

    return jax.shard_map(local, mesh=mesh, in_specs=in_specs, out_specs=out_specs, check_vma=False)
```

```python
import functools
import math

import jax
import jax.numpy as jnp
from jax import lax
from jax.experimental import pallas as pl
from jax.experimental.pallas import tpu as pltpu
from jax.sharding import PartitionSpec as P

KEY_VALUE_HEADS = 4
HEAD_WIDTH = 128
EXPERTS = 4
CHUNK = 512
RING = 5
EARLY = 3
IN_SPLIT = (2, 2, 2, 2)
OUT_SPLIT = (1, 2, 2, 3)
LAG = 1
LOADS = 4

norm_eps = 1e-05
MESH = pl.DeviceIdType.MESH


def attend(q_ref, fk_ref, fv_ref, k_ref, v_ref, ctx_ref, q_rows, att):
    reqs, features = q_ref.shape
    positions = k_ref.shape[1]
    heads = features // HEAD_WIDTH
    group = heads // KEY_VALUE_HEADS
    scale = 1.0 / math.sqrt(HEAD_WIDTH)
    q = q_ref[...].astype(jnp.float32)
    fk = fk_ref[...].astype(jnp.float32)
    fv = fv_ref[...].astype(jnp.float32)
    for r in range(reqs):
        for h in range(heads):
            q_rows[r * heads + h : r * heads + h + 1, :] = q[
                r : r + 1, h * HEAD_WIDTH : (h + 1) * HEAD_WIDTH
            ]
    scores, own, valid = [], [], []
    position = lax.broadcasted_iota(jnp.int32, (heads, positions), 1)
    for r in range(reqs):
        valid.append(position < ctx_ref[r])
        for j in range(KEY_VALUE_HEADS):
            rows = slice(r * heads + j * group, r * heads + (j + 1) * group)
            cols = slice(j * HEAD_WIDTH, (j + 1) * HEAD_WIDTH)
            qj = q_rows[rows, :]
            scores.append(
                lax.dot_general(
                    qj.astype(jnp.bfloat16),
                    k_ref[r, :, cols],
                    (((1,), (1,)), ((), ())),
                    preferred_element_type=jnp.float32,
                )
            )
            own.append(jnp.sum(qj * fk[r : r + 1, cols], axis=1, keepdims=True))
    ok = jnp.concatenate(valid, axis=0)
    s = jnp.concatenate(scores, axis=0) * scale
    o = jnp.concatenate(own, axis=0) * scale
    m = jnp.maximum(jnp.max(jnp.where(ok, s, -1e30), axis=1, keepdims=True), o)
    e = jnp.where(ok, jnp.exp(s - m), 0.0)
    oe = jnp.exp(o - m)
    total = jnp.sum(e, axis=1, keepdims=True) + oe
    w = (e / total).astype(jnp.bfloat16)
    ow = (oe / total).astype(jnp.bfloat16).astype(jnp.float32)
    for r in range(reqs):
        for j in range(KEY_VALUE_HEADS):
            rows = slice(r * heads + j * group, r * heads + (j + 1) * group)
            cols = slice(j * HEAD_WIDTH, (j + 1) * HEAD_WIDTH)
            mixed = jnp.dot(w[rows], v_ref[r, :, cols], preferred_element_type=jnp.float32)
            mixed = mixed + ow[rows] * fv[r : r + 1, cols]
            for g in range(group):
                h = j * group + g
                att[r : r + 1, h * HEAD_WIDTH : (h + 1) * HEAD_WIDTH] = mixed[g : g + 1, :]


def cut(total, split):
    unit = total // sum(split)
    sizes = [unit * part for part in split]
    return [(sum(sizes[:i]), size) for i, size in enumerate(sizes)]


def shared_kernel(groups, n, *refs):
    small_hbm, refs = refs[:10], refs[10:]
    small, refs = refs[4:14], refs[:4] + refs[14:]
    wg_hbm, wu_hbm, wd_hbm, out_ref, w, wd, q_rows, residual, acc, hidden = refs[:10]
    refs = refs[10:]
    ins, outs = len(IN_SPLIT), len(OUT_SPLIT)
    xs, xd, xf, x32s = (refs[ins * i : ins * (i + 1)] for i in range(4))
    refs = refs[4 * ins :]
    keep, ps, pr, ys, yr = (refs[outs * i : outs * (i + 1)] for i in range(5))
    (
        in_sem,
        w_sem,
        x_send,
        x_recv,
        f_send,
        f_recv,
        p_send,
        p_recv,
        y_send,
        y_recv,
    ) = refs[5 * outs :]
    ctx_ref, res_ref, q_ref, fk_ref, fv_ref, gain_ref, ids_ref, gates_ref, k_buf, v_buf = small
    g, e = lax.axis_index("groups"), lax.axis_index("ep")
    per_group = n // 2
    chips = groups * per_group
    core = lax.rem(e, 2)
    chip = g * per_group + e // 2
    partner = {"groups": g, "ep": e + 1 - 2 * core}
    reqs, features = res_ref.shape
    units = wd.shape[0]
    in_parts, out_parts = cut(features, IN_SPLIT), cut(features, OUT_SPLIT)
    rows = chips * reqs

    place = e // 2

    def turned(at, by, size):
        moved = at + by
        return moved - jnp.where(moved >= size, size, 0)

    targets = []
    near = sorted(range(per_group), key=lambda t: abs(t - per_group // 2))
    for t in near:
        for s in reversed(range(groups)):
            to_group, to_place = turned(g, s, groups), turned(place, t, per_group)
            targets.append(
                (
                    to_group * per_group + to_place,
                    {"groups": to_group, "ep": to_place * 2 + 1 - core},
                )
            )

    owners = []
    for q in sorted(range(chips), key=lambda q: (q // per_group) + (q % per_group)):
        owners.append((q, {"groups": q // per_group, "ep": (q % per_group) * 2 + 1 - core}))

    barrier = pltpu.get_barrier_semaphore()
    for _, device in targets:
        pl.semaphore_signal(barrier, inc=1, device_id=device, device_id_type=MESH)

    loads = [
        pltpu.make_async_copy(source, target, in_sem.at[i])
        for i, (source, target) in enumerate(zip(small_hbm, small))
    ]
    for load in loads:
        load.start()

    first = pl.multiple_of(g * units, 128)

    mine = pl.ds(first, units)
    for i in range(LOADS):
        at = pl.ds(i * (features // LOADS), features // LOADS)
        pltpu.make_async_copy(
            wg_hbm.at[at, mine], w.at[at, pl.ds(0, units)], w_sem.at[0]
        ).start(priority=1)
        pltpu.make_async_copy(
            wu_hbm.at[at, mine], w.at[at, pl.ds(units, units)], w_sem.at[0]
        ).start(priority=1)
    for i in range(LOADS):
        at = pl.ds(i * (units // LOADS), units // LOADS)
        pltpu.make_async_copy(
            wd_hbm.at[pl.ds(pl.multiple_of(first + i * (units // LOADS), 128), units // LOADS), :],
            wd.at[at, :],
            w_sem.at[1],
        ).start(priority=1)

    for load in loads:
        load.wait()
    attend(q_ref, fk_ref, fv_ref, k_buf, v_buf, ctx_ref, q_rows, residual)
    full = res_ref[...].astype(jnp.float32) + residual[...]
    residual[...] = full
    factor = lax.rsqrt(jnp.mean(full * full, axis=1, keepdims=True) + norm_eps)
    normed = (full * factor * gain_ref[...]).astype(jnp.bfloat16)
    for k, (start, size) in enumerate(in_parts):
        xs[k][...] = normed[:, start : start + size]

    pl.semaphore_wait(barrier, chips)

    for k in range(ins):
        for _, device in targets:
            pltpu.make_async_remote_copy(
                src_ref=xs[k],
                dst_ref=xd[k].at[chip],
                send_sem=x_send.at[k],
                recv_sem=x_recv.at[k],
                device_id=device,
                device_id_type=MESH,
            ).start()

    def wait_for(ref, sem):
        pltpu.make_async_copy(ref, ref, sem).wait()

    def forward(k):
        return pltpu.make_async_remote_copy(
            src_ref=xd[k],
            dst_ref=xf[k],
            send_sem=f_send.at[k],
            recv_sem=f_recv.at[k],
            device_id=partner,
            device_id_type=MESH,
        )

    def pass_on(k):
        wait_for(xd[k], x_recv.at[k])
        forward(k).start()

    pass_on(0)
    for k, (start, size) in enumerate(in_parts):
        if k + 1 < ins:
            pass_on(k + 1)
        forward(k).wait_recv()
        x32 = x32s[k]
        for q in range(chips):
            x32[reqs * q : reqs * (q + 1), :] = xd[k][q].astype(jnp.float32)
            x32[rows + reqs * q : rows + reqs * (q + 1), :] = xf[k][q].astype(jnp.float32)
        x = x32[...].astype(jnp.bfloat16)
        if k == 0:
            wait_for(w, w_sem.at[0])
        term = jnp.dot(x, w[start : start + size, :], preferred_element_type=jnp.float32)
        if k == 0:
            acc[...] = term
        else:
            acc[...] += term

    gate = acc[:, 0:units]
    hidden[...] = (gate / (1.0 + jnp.exp(-gate)) * acc[:, units:]).astype(jnp.bfloat16)

    def give(j):
        return pltpu.make_async_remote_copy(
            src_ref=ps[j],
            dst_ref=pr[j],
            send_sem=p_send.at[j],
            recv_sem=p_recv.at[j],
            device_id=partner,
            device_id_type=MESH,
        )

    def send_back(j):
        give(j).wait_recv()
        both = (keep[j][...] + pr[j][...].astype(jnp.float32)).astype(jnp.bfloat16)
        for q in range(chips):
            ys[j][q] = both[reqs * q : reqs * (q + 1)]

        for q, device in owners:
            pltpu.make_async_remote_copy(
                src_ref=ys[j].at[q],
                dst_ref=yr[j].at[chip],
                send_sem=y_send.at[j],
                recv_sem=y_recv.at[j],
                device_id=device,
                device_id_type=MESH,
            ).start()

    wait_for(wd, w_sem.at[1])
    for j in range(outs + LAG):
        if j < outs:
            start, size = out_parts[j]
            part = jnp.dot(
                hidden[...], wd[:, start : start + size], preferred_element_type=jnp.float32
            )
            ps[j][...] = part[rows:].astype(jnp.bfloat16)
            give(j).start()
            keep[j][...] = part[0:rows]
        if j >= LAG:
            send_back(j - LAG)

    ids = ids_ref[...]
    gates = gates_ref[...].astype(jnp.float32)
    per_expert = per_group // EXPERTS
    weights = []
    for expert in range(EXPERTS):
        weights.append(jnp.sum(jnp.where(ids == expert, gates, 0.0), axis=1, keepdims=True))

    for j, (start, size) in enumerate(out_parts):
        cols = slice(start, start + size)
        wait_for(yr[j], y_recv.at[j])
        total = residual[:, cols]
        for expert in range(EXPERTS):
            share = None
            for group in range(groups):
                for i in range(per_expert):
                    term = yr[j][group * per_group + expert * per_expert + i].astype(jnp.float32)
                    share = term if share is None else share + term
            total = total + weights[expert] * share
        out_ref[:, cols] = total.astype(out_ref.dtype)

    for k in range(ins):
        wait_for(xd[k], x_send.at[k])
        forward(k).wait_send()
    for j in range(outs):
        give(j).wait_send()
        wait_for(ys[j], y_send.at[j])


def shared_local(
    residual_in,
    queries,
    fresh_keys,
    fresh_values,
    stored_keys,
    stored_values,
    context_len,
    norm_gain,
    expert_ids,
    expert_gates,
    gate_weight,
    up_weight,
    down_weight,
):
    groups, n = lax.axis_size("groups"), lax.axis_size("ep")
    reqs, features = residual_in.shape
    units = gate_weight.shape[1] // groups
    chips = groups * n // 2
    rows = chips * reqs
    in_sizes = [size for _, size in cut(features, IN_SPLIT)]
    out_sizes = [size for _, size in cut(features, OUT_SPLIT)]
    bf16, f32 = jnp.bfloat16, jnp.float32
    vmem = pl.BlockSpec(memory_space=pltpu.VMEM)
    hbm = pl.BlockSpec(memory_space=pltpu.HBM)
    dma = pltpu.SemaphoreType.DMA
    return pl.pallas_call(
        functools.partial(shared_kernel, groups, n),
        out_shape=jax.ShapeDtypeStruct((reqs, features), bf16),
        in_specs=[hbm] * 13,
        out_specs=vmem,
        scratch_shapes=[
            pltpu.SMEM(context_len.shape, jnp.int32),
            pltpu.VMEM((reqs, features), bf16),
            pltpu.VMEM((reqs, features), bf16),
            pltpu.VMEM(fresh_keys.shape, bf16),
            pltpu.VMEM(fresh_values.shape, bf16),
            pltpu.VMEM((1, features), f32),
            pltpu.VMEM(expert_ids.shape, jnp.int32),
            pltpu.VMEM(expert_gates.shape, bf16),
            pltpu.VMEM(stored_keys.shape, bf16),
            pltpu.VMEM(stored_values.shape, bf16),
            pltpu.VMEM((features, 2 * units), bf16),
            pltpu.VMEM((units, features), bf16),
            pltpu.VMEM((reqs * features // HEAD_WIDTH, HEAD_WIDTH), f32),
            pltpu.VMEM((reqs, features), f32),
            pltpu.VMEM((2 * rows, 2 * units), f32),
            pltpu.VMEM((2 * rows, units), bf16),
            *(pltpu.VMEM((reqs, size), bf16) for size in in_sizes),
            *(pltpu.VMEM((chips, reqs, size), bf16) for size in in_sizes),
            *(pltpu.VMEM((chips, reqs, size), bf16) for size in in_sizes),
            *(pltpu.VMEM((2 * rows, size), f32) for size in in_sizes),
            *(pltpu.VMEM((rows, size), f32) for size in out_sizes),
            *(pltpu.VMEM((rows, size), bf16) for size in out_sizes),
            *(pltpu.VMEM((rows, size), bf16) for size in out_sizes),
            *(pltpu.VMEM((chips, reqs, size), bf16) for size in out_sizes),
            *(pltpu.VMEM((chips, reqs, size), bf16) for size in out_sizes),
            dma((10,)),
            dma((2,)),
            *(dma((len(IN_SPLIT),)) for _ in range(4)),
            *(dma((len(OUT_SPLIT),)) for _ in range(4)),
        ],
        compiler_params=pltpu.CompilerParams(
            collective_id=0, has_side_effects=True, vmem_limit_bytes=66_000_000
        ),
        name="decode_step",
    )(
        context_len,
        residual_in,
        queries,
        fresh_keys,
        fresh_values,
        norm_gain.reshape(1, features),
        expert_ids,
        expert_gates,
        stored_keys,
        stored_values,
        gate_weight,
        up_weight,
        down_weight,
    )


def kernel(
    n,
    *refs,
):
    small_hbm, refs = refs[:10], refs[10:]
    small, refs = refs[4:14], refs[:4] + refs[14:]
    (
    wg_hbm,
    wu_hbm,
    wd_hbm,
    out_ref,
    wg,
    wu,
    wd,
    q_rows,
    residual,
    xr,
    x32,
    acc_g,
    acc_u,
    hidden,
    ys,
    yr,
    in_sem,
    g_sem,
    u_sem,
    d_sem,
    x_send,
    x_recv,
    y_send,
    y_recv,
    ) = refs
    ctx_ref, res_ref, q_ref, fk_ref, fv_ref, gain_ref, ids_ref, gates_ref, k_buf, v_buf = small
    me = lax.axis_index("ep")
    split = n // EXPERTS
    reqs, features = res_ref.shape
    k_steps = features // CHUNK
    ring = wg.shape[0]

    loads = [
        pltpu.make_async_copy(source, target, in_sem.at[i])
        for i, (source, target) in enumerate(zip(small_hbm, small))
    ]
    for load in loads:
        load.start()

    def gate_copy(step, slot):
        rows = pl.ds(pl.multiple_of(step * CHUNK, CHUNK), CHUNK)
        return pltpu.make_async_copy(wg_hbm.at[rows, :], wg.at[slot], g_sem.at[slot])

    def up_copy(step, slot):
        rows = pl.ds(pl.multiple_of(step * CHUNK, CHUNK), CHUNK)
        return pltpu.make_async_copy(wu_hbm.at[rows, :], wu.at[slot], u_sem.at[slot])

    def down_copy(step):
        cols = pl.ds(pl.multiple_of(step * CHUNK, CHUNK), CHUNK)
        return pltpu.make_async_copy(wd_hbm.at[:, cols], wd.at[step], d_sem.at[step])

    early = min(EARLY, k_steps)
    for step in range(ring):
        gate_copy(step, step).start(priority=1)
        up_copy(step, step).start(priority=1)
    for step in range(early):
        down_copy(step).start(priority=1)

    barrier = pltpu.get_barrier_semaphore()

    @pl.loop(1, n)
    def _(d):
        pl.semaphore_signal(
            barrier, inc=1, device_id={"ep": lax.rem(me + d, n)}, device_id_type=MESH
        )

    acc_g[...] = jnp.zeros_like(acc_g)
    acc_u[...] = jnp.zeros_like(acc_u)
    for load in loads:
        load.wait()
    attend(q_ref, fk_ref, fv_ref, k_buf, v_buf, ctx_ref, q_rows, residual)
    full = res_ref[...].astype(jnp.float32) + residual[...]
    residual[...] = full
    factor = lax.rsqrt(jnp.mean(full * full, axis=1, keepdims=True) + norm_eps)
    normed = (full * factor * gain_ref[...]).astype(jnp.bfloat16)
    for k in range(k_steps):
        xr[k, 0] = normed[:, k * CHUNK : (k + 1) * CHUNK]

    pl.semaphore_wait(barrier, n - 1)

    ahead = k_steps

    def send_rows(k):
        @pl.loop(1, n)
        def _(d):
            pltpu.make_async_remote_copy(
                src_ref=xr.at[k, 0],
                dst_ref=xr.at[k, d],
                send_sem=x_send.at[k],
                recv_sem=x_recv.at[k],
                device_id={"ep": lax.rem(me + d, n)},
                device_id_type=MESH,
            ).start()

    for k in range(ahead):
        send_rows(k)

    def wait_blocks(ref, sem):
        pltpu.make_async_copy(ref, ref, sem).wait()

    @pl.loop(0, k_steps)
    def _(k):
        slot = lax.rem(k, ring)

        @pl.when(k + ahead < k_steps)
        def _():
            send_rows(k + ahead)

        wait_blocks(xr.at[k, pl.ds(1, n - 1)], x_recv.at[k])
        for d in range(n):
            x32[reqs * d : reqs * (d + 1), :] = xr[k, d].astype(jnp.float32)
        x = x32[...].astype(jnp.bfloat16)
        gate_copy(k, slot).wait()
        acc_g[...] += jnp.dot(x, wg[slot], preferred_element_type=jnp.float32)
        up_copy(k, slot).wait()
        acc_u[...] += jnp.dot(x, wu[slot], preferred_element_type=jnp.float32)

        @pl.when(k + ring < k_steps)
        def _():
            gate_copy(k + ring, slot).start(priority=1)
            up_copy(k + ring, slot).start(priority=1)

        @pl.when(k == max(k_steps - ring - 1, 0))
        def _():
            @pl.loop(early, k_steps)
            def _(j):
                down_copy(j).start(priority=1)

    gate = acc_g[...]
    hidden[...] = (gate / (1.0 + jnp.exp(-gate)) * acc_u[...]).astype(jnp.bfloat16)

    @pl.loop(0, k_steps)
    def _(j):
        down_copy(j).wait()
        part = jnp.dot(hidden[...], wd[j], preferred_element_type=jnp.float32)
        yr[j, 0] = part[0:reqs].astype(jnp.bfloat16)
        for d in range(1, n):
            ys[j, d] = part[reqs * d : reqs * (d + 1)].astype(jnp.bfloat16)

        @pl.loop(1, n)
        def _(d):
            pltpu.make_async_remote_copy(
                src_ref=ys.at[j, d],
                dst_ref=yr.at[j, d],
                send_sem=y_send.at[j],
                recv_sem=y_recv.at[j],
                device_id={"ep": lax.rem(me - d + n, n)},
                device_id_type=MESH,
            ).start()

    ids = ids_ref[...]
    gates = gates_ref[...].astype(jnp.float32)
    weights = []
    for expert in range(EXPERTS):
        weights.append(jnp.sum(jnp.where(ids == expert, gates, 0.0), axis=1, keepdims=True))

    for j in range(k_steps):
        cols = slice(j * CHUNK, (j + 1) * CHUNK)
        wait_blocks(yr.at[j, pl.ds(1, n - 1)], y_recv.at[j])
        total = residual[:, cols]
        for d in range(n):
            expert = lax.rem(me + d, n) // split
            weight = weights[0]
            for other in range(1, EXPERTS):
                weight = jnp.where(expert == other, weights[other], weight)
            total = total + weight * yr[j, d].astype(jnp.float32)
        out_ref[:, cols] = total.astype(out_ref.dtype)

    @pl.loop(0, k_steps)
    def _(k):
        wait_blocks(xr.at[k, pl.ds(1, n - 1)], x_send.at[k])
        wait_blocks(ys.at[k, pl.ds(1, n - 1)], y_send.at[k])


def plain_local(
    residual_in,
    queries,
    fresh_keys,
    fresh_values,
    stored_keys,
    stored_values,
    context_len,
    norm_gain,
    expert_ids,
    expert_gates,
    gate_weight,
    up_weight,
    down_weight,
):
    n = lax.axis_size("ep")
    reqs, features = residual_in.shape
    units = gate_weight.shape[1]
    steps = features // CHUNK
    ring = min(RING, steps)
    bf16, f32 = jnp.bfloat16, jnp.float32
    vmem = pl.BlockSpec(memory_space=pltpu.VMEM)
    hbm = pl.BlockSpec(memory_space=pl.ANY)
    dma = pltpu.SemaphoreType.DMA
    rows = n * reqs
    return pl.pallas_call(
        functools.partial(kernel, n),
        out_shape=jax.ShapeDtypeStruct((reqs, features), bf16),
        in_specs=[hbm] * 13,
        out_specs=vmem,
        scratch_shapes=[
            pltpu.SMEM(context_len.shape, jnp.int32),
            pltpu.VMEM((reqs, features), bf16),
            pltpu.VMEM((reqs, features), bf16),
            pltpu.VMEM(fresh_keys.shape, bf16),
            pltpu.VMEM(fresh_values.shape, bf16),
            pltpu.VMEM((1, features), f32),
            pltpu.VMEM(expert_ids.shape, jnp.int32),
            pltpu.VMEM(expert_gates.shape, bf16),
            pltpu.VMEM(stored_keys.shape, bf16),
            pltpu.VMEM(stored_values.shape, bf16),
            pltpu.VMEM((ring, CHUNK, units), bf16),
            pltpu.VMEM((ring, CHUNK, units), bf16),
            pltpu.VMEM((steps, units, CHUNK), bf16),
            pltpu.VMEM((reqs * features // HEAD_WIDTH, HEAD_WIDTH), f32),
            pltpu.VMEM((reqs, features), f32),
            pltpu.VMEM((steps, n, reqs, CHUNK), bf16),
            pltpu.VMEM((rows, CHUNK), f32),
            pltpu.VMEM((rows, units), f32),
            pltpu.VMEM((rows, units), f32),
            pltpu.VMEM((rows, units), bf16),
            pltpu.VMEM((steps, n, reqs, CHUNK), bf16),
            pltpu.VMEM((steps, n, reqs, CHUNK), bf16),
            dma((10,)),
            dma((ring,)),
            dma((ring,)),
            dma((steps,)),
            dma((steps,)),
            dma((steps,)),
            dma((steps,)),
            dma((steps,)),
        ],
        compiler_params=pltpu.CompilerParams(
            collective_id=0, has_side_effects=True, vmem_limit_bytes=66_000_000
        ),
        name="decode_step",
    )(
        context_len,
        residual_in,
        queries,
        fresh_keys,
        fresh_values,
        norm_gain.reshape(1, features),
        expert_ids,
        expert_gates,
        stored_keys,
        stored_values,
        gate_weight,
        up_weight,
        down_weight,
    )


def solution(mesh):
    in_specs = (
        P(("groups", "ep"), None),
        P(("groups", "ep"), None),
        P(("groups", "ep"), None),
        P(("groups", "ep"), None),
        P(("groups", "ep"), None, None),
        P(("groups", "ep"), None, None),
        P(("groups", "ep")),
        P(),
        P(("groups", "ep"), None),
        P(("groups", "ep"), None),
        P(None, "ep"),
        P(None, "ep"),
        P("ep", None),
    )
    out_specs = P(("groups", "ep"), None)
    groups, n = mesh.shape["groups"], mesh.shape["ep"]

    def local(*args):
        units = args[10].shape[1]
        features = args[0].shape[1]
        split = max(sum(IN_SPLIT), sum(OUT_SPLIT))
        shared = n % (2 * EXPERTS) == 0 and units % (128 * groups) == 0
        shared = shared and features % (128 * split) == 0
        return (shared_local if shared else plain_local)(*args)

    return jax.shard_map(local, mesh=mesh, in_specs=in_specs, out_specs=out_specs, check_vma=False)
```
